512 devices in a mesh: dp: 32 (over y_lo, z), owner: 16 (over x, y_hi, core).
Axes of the slice: x: 4, y: 8 (y_hi: 2, y_lo: 4; y = y_hi * 4 + y_lo), z: 8, core: 2. Of those that a mesh axis runs over, the one named last changes fastest.
Arguments:
- gradients: bfloat16 [32, 16, 512, 512], P('dp', 'owner'), may hold values from -600 to 600
- block_layer: int32 [16], P('owner'), may hold values from 0 to 3
Outputs:
- update: bfloat16 [16, 512, 512], P('owner', 'dp')
The draws below stay inside these ranges and needn't reach their ends.
All inputs are finite; a program needn't handle non-finite values.
Results may differ from the reference program's by a relative error of at most 0.0062.
Values may be sent and summed in bfloat16 or wider, within the bound.
No kernel may reach another device: no remote copies, remote signals or barrier semaphores. Data moves between devices by JAX's collectives and lax.ppermute only.
A program may use at most 64 MiB of HBM per device.

```python
import math
import jax
import jax.numpy as jnp
from jax import lax

B = 512
LAYERS = 4
ITERS = 3
NBLK = 16
N_DP = 32


def draw_gradients(key, part):
    first_key = jax.random.fold_in(jax.random.fold_in(key, 11), 0)
    third_key = jax.random.fold_in(jax.random.fold_in(key, 11), 2)
    fourth_key = jax.random.fold_in(jax.random.fold_in(key, 11), 3)
    fifth_key = jax.random.fold_in(jax.random.fold_in(key, 11), 4)
    scales = jnp.exp(jax.random.uniform(first_key, (N_DP, NBLK, 1, 1), jnp.float32, 0.0, math.log(10.0)))
    heavy = jax.random.randint(fourth_key, (1, NBLK, 1, 1), 0, N_DP)
    replica_ids = jnp.arange(N_DP, dtype=jnp.int32)[:, None, None, None]
    scales = jnp.where(replica_ids == heavy, 25.0, scales)
    row_place = jnp.arange(B, dtype=jnp.float32)[None, None, :, None] / float(B - 1)
    jitter = jnp.exp(jax.random.uniform(fifth_key, (1, NBLK, B, 1), jnp.float32, math.log(0.8), math.log(1.25)))
    ramp = jnp.exp(0.5 * math.log(10.0) * row_place) * jitter
    values = jnp.clip(jax.random.normal(third_key, (N_DP, NBLK, B, B), jnp.float32), -6.0, 6.0)
    return (scales * ramp * values).astype(jnp.bfloat16)


def with_ends(array, stream_key, low, high):
    extent = array.shape
    place = [jax.random.randint(jax.random.fold_in(stream_key, axis), (), 0, extent[axis]) for axis in range(len(extent))]
    array = array.at[tuple(place)].set(low)
    longest = extent.index(max(extent))
    place[longest] = (place[longest] + 1) % extent[longest]
    return array.at[tuple(place)].set(high)


def setup_inputs(seed: int = 0) -> dict:
    arg_keys = jax.random.split(jax.random.key(seed), 3)
    return {
        "gradients": draw_gradients(jax.random.fold_in(arg_keys[2], 71), 0),
        "block_layer": with_ends(jax.random.randint(arg_keys[1], (NBLK,), 0, LAYERS), jax.random.fold_in(arg_keys[1], 1), 0, LAYERS - 1).astype(jnp.int32),
    }


def inverse_root(statistic):
    size_b = statistic.shape[0]
    identity = jnp.eye(size_b, dtype=jnp.float32)
    ridge_term = 0.01 * jnp.trace(statistic) / size_b + 1e-06
    shifted = statistic + ridge_term * identity
    scaling = jnp.sqrt(jnp.sum(shifted * shifted))
    current = shifted / scaling
    inverse = identity
    for step_number in range(ITERS):
        factor = (5.0 * identity - current) / 4.0
        if step_number == 0:
            inverse = scaling ** (-0.25) * factor
        else:
            inverse = jnp.dot(inverse, factor, precision=lax.Precision.HIGHEST)
        if step_number + 1 < ITERS:
            square = jnp.dot(factor, factor, precision=lax.Precision.HIGHEST)
            fourth = jnp.dot(square, square, precision=lax.Precision.HIGHEST)
            current = jnp.dot(fourth, current, precision=lax.Precision.HIGHEST)
    return inverse

def one_block(block_grads):
    widened = block_grads.astype(jnp.float32)
    left_sum = jnp.einsum('dij,dkj->ik', widened, widened, precision=lax.Precision.HIGHEST)
    right_sum = jnp.einsum('dji,djk->ik', widened, widened, precision=lax.Precision.HIGHEST)
    left_root = lax.optimization_barrier(inverse_root(left_sum).astype(jnp.bfloat16)).astype(jnp.float32)
    right_root = lax.optimization_barrier(inverse_root(right_sum).astype(jnp.bfloat16)).astype(jnp.float32)
    total_sum = lax.optimization_barrier(jnp.sum(widened, axis=0))
    middle = jnp.dot(left_root, total_sum, precision=lax.Precision.HIGHEST)
    return jnp.dot(middle, right_root, precision=lax.Precision.HIGHEST) / N_DP

def reference(gradients, block_layer):
    precond = lax.map(one_block, jnp.swapaxes(gradients, 0, 1))
    energy = lax.optimization_barrier(jnp.sum(precond * precond, axis=(1, 2)))
    selector = (block_layer[:, None] == jnp.arange(LAYERS, dtype=jnp.int32)[None, :]).astype(jnp.float32)
    layer_energy = lax.optimization_barrier(jnp.sum(selector * energy[:, None], axis=0))
    layer_count = lax.optimization_barrier(jnp.sum(selector, axis=0)) * float(B * B)
    block_mean = lax.optimization_barrier(jnp.sum(selector * layer_energy[None, :], axis=1)) / lax.optimization_barrier(jnp.sum(selector * layer_count[None, :], axis=1))
    return (precond * lax.rsqrt(block_mean + 1e-06)[:, None, None]).astype(jnp.bfloat16)
```

```python
import jax
import jax.numpy as jnp
from jax import lax
from jax.experimental import pallas as pl
from jax.experimental.pallas import tpu as pltpu
from jax.sharding import Mesh
from jax.sharding import PartitionSpec as P

DP = ("dp_0", "dp_1")
OWNER = ("owner_0", "owner_1", "owner_2")
B = 512
H = B // 2
LANE = 128
N_DP = 32
N_OWNER = 16
ROWS = B // N_DP
COLS = B // LANE
BODY = ROWS * COLS
DIAG = 8


def dot(a, b, contract=((1,), (0,))):
    return lax.dot_general(a, b, (contract, ((), ())), preferred_element_type=jnp.float32)


def triangle():
    row = lax.broadcasted_iota(jnp.int32, (H, H), 0)
    col = lax.broadcasted_iota(jnp.int32, (H, H), 1)
    return row, col


def pack_kernel(grad_ref, out_ref):
    grad = grad_ref[...]
    row, col = triangle()
    diagonals = []
    for stat in range(2):
        if stat == 0:
            first, second, contract = grad[:H], grad[H:], ((1,), (1,))
        else:
            first, second, contract = grad[:, :H], grad[:, H:], ((0,), (0,))
        upper = dot(first, first, contract)
        cross = dot(first, second, contract)
        lower = dot(second, second, contract)
        folded = jnp.where(row <= col, upper, lower).astype(jnp.bfloat16)
        cross = cross.astype(jnp.bfloat16)
        diagonal = jnp.sum(jnp.where(row == col, lower, 0.0), axis=0, keepdims=True)
        diagonals += [diagonal[:, :LANE], diagonal[:, LANE:]]
        slots = pl.ds(stat * N_DP // 2, N_DP // 2)
        for c, part in enumerate((cross[:, :LANE], cross[:, LANE:], folded[:, :LANE], folded[:, LANE:])):
            out_ref[slots, c * ROWS : (c + 1) * ROWS, :] = part.reshape(N_DP // 2, ROWS, LANE)
    out_ref[:, BODY : BODY + DIAG, :] = jnp.zeros((N_DP, DIAG, LANE), jnp.bfloat16)
    extra = jnp.concatenate(diagonals + [jnp.zeros((DIAG - 4, LANE), jnp.float32)], axis=0)
    out_ref[0, BODY : BODY + DIAG, :] = extra.astype(jnp.bfloat16)
    for c in range(COLS):
        start = BODY + DIAG + c * ROWS
        out_ref[:, start : start + ROWS, :] = grad[:, c * LANE : (c + 1) * LANE].reshape(N_DP, ROWS, LANE)


def inverse_root(statistic_parts, row, col):
    upper, cross, lower = statistic_parts
    on_diagonal = row == col
    trace = jnp.sum(jnp.where(on_diagonal, upper + lower, 0.0))
    ridge = 0.01 * trace / B + 1e-06
    upper = jnp.where(on_diagonal, upper + ridge, upper)
    lower = jnp.where(on_diagonal, lower + ridge, lower)
    total = jnp.sum(upper * upper + 2.0 * (cross * cross) + lower * lower)
    total = jnp.broadcast_to(total, (1, LANE))
    inverse_scale = lax.rsqrt(total)[:, :1]
    root_scale = jnp.exp(jnp.log(total) * -0.125)[:, :1]
    current = jnp.concatenate(
        [jnp.concatenate([upper, cross], axis=1), jnp.concatenate([cross.T, lower], axis=1)], axis=0
    ) * inverse_scale

    def advance(m):
        mb = m.astype(jnp.bfloat16)
        u = dot(mb, mb) * 0.0625 - 0.625 * m
        ub = u.astype(jnp.bfloat16)
        v = dot(ub, ub) + 3.125 * u
        return mb, dot(v.astype(jnp.bfloat16), mb) + 2.44140625 * m

    mb, second = advance(current)
    sb, third = advance(second)
    y = dot(mb, sb) * 0.0625 - 0.3125 * (current + second)
    tb = third.astype(jnp.bfloat16)
    z = dot(y.astype(jnp.bfloat16), tb)
    rest = 1.25 * y - 0.390625 * third - 0.25 * z
    full_row = lax.broadcasted_iota(jnp.int32, (B, B), 0)
    full_col = lax.broadcasted_iota(jnp.int32, (B, B), 1)
    return (jnp.where(full_row == full_col, rest + 1.953125, rest) * root_scale).astype(jnp.bfloat16)


def roots_kernel(stat_ref, left_ref, right_ref):
    row, col = triangle()
    for stat, out_ref in enumerate((left_ref, right_ref)):
        slots = pl.ds(stat * N_DP // 2, N_DP // 2)
        parts = [
            stat_ref[slots, c * ROWS : (c + 1) * ROWS, :].reshape(H, LANE).astype(jnp.float32)
            for c in range(COLS)
        ]
        cross = jnp.concatenate(parts[:2], axis=1)
        folded = jnp.concatenate(parts[2:], axis=1)
        flipped = folded.T
        extra = stat_ref[0, BODY : BODY + DIAG, :].astype(jnp.float32)
        diagonal = jnp.concatenate([extra[2 * stat : 2 * stat + 1], extra[2 * stat + 1 : 2 * stat + 2]], axis=1)
        upper = jnp.where(row <= col, folded, flipped)
        lower = jnp.where(row > col, folded, flipped)
        lower = jnp.where(row == col, diagonal, lower)
        out_ref[...] = inverse_root((upper, cross, lower), row, col)


def apply_kernel(place_ref, layer_ref, total_ref, left_ref, right_ref, rows_ref, note_ref, whole_ref):
    right = right_ref[...]
    total = jnp.concatenate(
        [total_ref[:, c * ROWS : (c + 1) * ROWS, :].reshape(B, LANE) for c in range(COLS)], axis=1
    )
    middle = dot(left_ref[...], total)
    high = middle.astype(jnp.bfloat16)
    low = (middle - high.astype(jnp.float32)).astype(jnp.bfloat16)
    whole = (dot(high, right) + dot(low, right)) * (1.0 / N_DP)
    whole_ref[...] = whole
    energy = jnp.sum(whole * whole)
    lane = lax.broadcasted_iota(jnp.int32, note_ref.shape, 2)
    note_ref[...] = jnp.where(lane == 0, energy, layer_ref[0].astype(jnp.float32))
    rows_ref[...] = whole_ref[pl.ds(place_ref[0] * ROWS, ROWS), :]


def scale_kernel(layer_ref, notes_ref, rows_ref, out_ref):
    notes = notes_ref[...]
    mine = notes[:, 0, 1:2] == layer_ref[0].astype(jnp.float32)
    energy = jnp.sum(jnp.where(mine, notes[:, 0, 0:1], 0.0), axis=0, keepdims=True)
    count = jnp.sum(jnp.where(mine, float(B * B), 0.0), axis=0, keepdims=True)
    out_ref[...] = (rows_ref[...] * lax.rsqrt(energy / count + 1e-06)).astype(jnp.bfloat16)


VMEM = pl.BlockSpec(memory_space=pltpu.VMEM)
SMEM = pl.BlockSpec(memory_space=pltpu.SMEM)


def shape(dims, dtype):
    return jax.ShapeDtypeStruct(dims, dtype)


def to_all(x, axes, size):
    return lax.all_to_all(jnp.broadcast_to(x[None], (size, *x.shape)), axes, 0, 0, tiled=True)


def per_device(gradients, block_layer):
    packed = pl.pallas_call(
        pack_kernel,
        out_shape=shape((N_DP, 2 * BODY + DIAG, LANE), jnp.bfloat16),
        in_specs=[VMEM],
        out_specs=VMEM,
        name="pack",
    )(gradients[0, 0])
    arrived = lax.all_to_all(packed, DP, 0, 0, tiled=True)
    mine = jnp.sum(arrived.astype(jnp.float32), axis=0).astype(jnp.bfloat16)
    stats = to_all(mine[: BODY + DIAG], DP, N_DP)
    stats, total = lax.optimization_barrier((stats, mine[BODY + DIAG :]))
    total = to_all(total, DP, N_DP)
    left, right = pl.pallas_call(
        roots_kernel,
        out_shape=(shape((B, B), jnp.bfloat16), shape((B, B), jnp.bfloat16)),
        in_specs=[VMEM],
        out_specs=(VMEM, VMEM),
        cost_estimate=pl.CostEstimate(flops=10 * 16 * 2 * B**3, bytes_accessed=2 * B * B * 4, transcendentals=0),
        name="roots",
    )(stats)
    place = lax.axis_index(DP)[None].astype(jnp.int32)
    rows, note = pl.pallas_call(
        apply_kernel,
        out_shape=(shape((ROWS, B), jnp.float32), shape((N_OWNER, 1, LANE), jnp.float32)),
        in_specs=[SMEM, SMEM, VMEM, VMEM, VMEM],
        out_specs=(VMEM, VMEM),
        scratch_shapes=[pltpu.VMEM((B, B), jnp.float32)],
        name="apply",
    )(place, block_layer, total, left, right)
    notes = lax.all_to_all(note, OWNER, 0, 0, tiled=True)
    update = pl.pallas_call(
        scale_kernel,
        out_shape=shape((ROWS, B), jnp.bfloat16),
        in_specs=[SMEM, VMEM, VMEM],
        out_specs=VMEM,
        name="scale",
    )(block_layer, notes, rows)
    return update[None]


def solution(mesh):
    finer = Mesh(
        mesh.devices.reshape(4, 8, 4, 2, 2), ("dp_0", "dp_1", "owner_0", "owner_1", "owner_2")
    )
    in_specs = (P(DP, OWNER, None, None), P(OWNER))
    out_specs = P(OWNER, DP, None)
    return jax.shard_map(
        per_device, mesh=finer, in_specs=in_specs, out_specs=out_specs, check_vma=False
    )
```

```python
import jax
import jax.numpy as jnp
from jax import lax
from jax.experimental import pallas as pl
from jax.experimental.pallas import tpu as pltpu
from jax.sharding import Mesh
from jax.sharding import PartitionSpec as P

DP = ("q", "p", "z")
OWNER = ("x", "h", "c")
PEERS = ("q", "z")
CHIP_PAIR = ("p", "c")
NOTE_AXES = ("q", "p", "x", "h", "c")
B = 512
H = B // 2
LANE = 128
N_DP = 32
N_PEER = 16
N_NOTE = 32
ROWS = B // N_DP
SLAB = H // N_PEER
COLS = B // LANE
BODY = SLAB * COLS
DIAG = 8


def dot(a, b, contract=((1,), (0,))):
    return lax.dot_general(a, b, (contract, ((), ())), preferred_element_type=jnp.float32)


def triangle():
    row = lax.broadcasted_iota(jnp.int32, (H, H), 0)
    col = lax.broadcasted_iota(jnp.int32, (H, H), 1)
    return row, col


def pack_kernel(role_ref, one_ref, two_ref, out_ref):
    row, col = triangle()

    def pack(role):
        upper = cross = lower = 0.0
        for ref in (one_ref, two_ref):
            if role == 0:
                first, second, contract = ref[:H], ref[H:], ((1,), (1,))
            else:
                first, second, contract = ref[:, :H], ref[:, H:], ((0,), (0,))
            upper += dot(first, first, contract)
            cross += dot(first, second, contract)
            lower += dot(second, second, contract)
        folded = jnp.where(row <= col, upper, lower).astype(jnp.bfloat16)
        cross = cross.astype(jnp.bfloat16)
        diagonal = jnp.sum(jnp.where(row == col, lower, 0.0), axis=0, keepdims=True)
        for c, part in enumerate((cross[:, :LANE], cross[:, LANE:], folded[:, :LANE], folded[:, LANE:])):
            out_ref[:, c * SLAB : (c + 1) * SLAB, :] = part.reshape(N_PEER, SLAB, LANE)
        out_ref[:, BODY : BODY + DIAG, :] = jnp.zeros((N_PEER, DIAG, LANE), jnp.bfloat16)
        extra = jnp.concatenate(
            [diagonal[:, :LANE], diagonal[:, LANE:], jnp.zeros((DIAG - 2, LANE), jnp.float32)], axis=0
        )
        out_ref[0, BODY : BODY + DIAG, :] = extra.astype(jnp.bfloat16)
        half = slice(role * H, (role + 1) * H)
        total = (one_ref[half].astype(jnp.float32) + two_ref[half].astype(jnp.float32)).astype(jnp.bfloat16)
        for c in range(COLS):
            start = BODY + DIAG + c * SLAB
            out_ref[:, start : start + SLAB, :] = total[:, c * LANE : (c + 1) * LANE].reshape(N_PEER, SLAB, LANE)

    for role in range(2):
        pl.when(role_ref[0] == role)(lambda role=role: pack(role))


def inverse_root(statistic_parts, row, col):
    upper, cross, lower = statistic_parts
    on_diagonal = row == col
    trace = jnp.sum(jnp.where(on_diagonal, upper + lower, 0.0))
    ridge = 0.01 * trace / B + 1e-06
    upper = jnp.where(on_diagonal, upper + ridge, upper)
    lower = jnp.where(on_diagonal, lower + ridge, lower)
    total = jnp.sum(upper * upper + 2.0 * (cross * cross) + lower * lower)
    total = jnp.broadcast_to(total, (1, LANE))
    inverse_scale = lax.rsqrt(total)[:, :1]
    root_scale = jnp.exp(jnp.log(total) * -0.125)[:, :1]
    current = jnp.concatenate(
        [jnp.concatenate([upper, cross], axis=1), jnp.concatenate([cross.T, lower], axis=1)], axis=0
    ) * inverse_scale

    def advance(m):
        mb = m.astype(jnp.bfloat16)
        u = dot(mb, mb) * 0.0625 - 0.625 * m
        ub = u.astype(jnp.bfloat16)
        v = dot(ub, ub) + 3.125 * u
        return mb, dot(v.astype(jnp.bfloat16), mb) + 2.44140625 * m

    mb, second = advance(current)
    sb, third = advance(second)
    y = dot(mb, sb) * 0.0625 - 0.3125 * (current + second)
    tb = third.astype(jnp.bfloat16)
    z = dot(y.astype(jnp.bfloat16), tb)
    rest = 1.25 * y - 0.390625 * third - 0.25 * z
    full_row = lax.broadcasted_iota(jnp.int32, (B, B), 0)
    full_col = lax.broadcasted_iota(jnp.int32, (B, B), 1)
    return (jnp.where(full_row == full_col, rest + 1.953125, rest) * root_scale).astype(jnp.bfloat16)


def root_kernel(stat_ref, out_ref):
    row, col = triangle()
    parts = [
        stat_ref[:, c * SLAB : (c + 1) * SLAB, :].reshape(H, LANE).astype(jnp.float32)
        for c in range(COLS)
    ]
    cross = jnp.concatenate(parts[:2], axis=1)
    folded = jnp.concatenate(parts[2:], axis=1)
    flipped = folded.T
    extra = stat_ref[0, BODY : BODY + DIAG, :].astype(jnp.float32)
    diagonal = jnp.concatenate([extra[0:1], extra[1:2]], axis=1)
    upper = jnp.where(row <= col, folded, flipped)
    lower = jnp.where(row > col, folded, flipped)
    lower = jnp.where(row == col, diagonal, lower)
    out_ref[...] = inverse_root((upper, cross, lower), row, col)


def apply_kernel(scalar_ref, mine_ref, half_ref, root_ref, other_ref, rows_ref, note_ref, whole_ref):
    role = scalar_ref[0]
    start = BODY + DIAG

    def wide(ref, offset):
        return jnp.concatenate(
            [
                ref[:, offset + c * SLAB : offset + (c + 1) * SLAB, :].reshape(H, LANE)
                for c in range(COLS)
            ],
            axis=1,
        )

    def apply(left_ref, right_ref, top, bottom):
        right = right_ref[...]
        middle = dot(left_ref[:, :H], top) + dot(left_ref[:, H:], bottom)
        high = middle.astype(jnp.bfloat16)
        low = (middle - high.astype(jnp.float32)).astype(jnp.bfloat16)
        whole = (dot(high, right) + dot(low, right)) * (1.0 / N_DP)
        whole_ref[...] = whole
        energy = jnp.sum(whole * whole)
        lane = lax.broadcasted_iota(jnp.int32, note_ref.shape, 2)
        layer = scalar_ref[2].astype(jnp.float32)
        note_ref[...] = jnp.where(lane == 0, energy, layer)

    @pl.when(role == 0)
    def _():
        apply(root_ref, other_ref, wide(mine_ref, start), wide(half_ref, 0))

    @pl.when(role == 1)
    def _():
        apply(other_ref, root_ref, wide(half_ref, 0), wide(mine_ref, start))

    rows_ref[...] = whole_ref[pl.ds(scalar_ref[1] * ROWS, ROWS), :]


def scale_kernel(scalar_ref, notes_ref, rows_ref, moved_ref, out_ref):
    notes = notes_ref[...]
    mine = notes[:, 0, 1:2] == scalar_ref[0].astype(jnp.float32)
    energy = jnp.sum(jnp.where(mine, notes[:, 0, 0:1], 0.0), axis=0, keepdims=True)
    count = jnp.sum(jnp.where(mine, float(B * B), 0.0), axis=0, keepdims=True)
    rows = jnp.where(scalar_ref[1] == 1, rows_ref[...], moved_ref[...])
    out_ref[...] = (rows * lax.rsqrt(energy / count + 1e-06)).astype(jnp.bfloat16)


VMEM = pl.BlockSpec(memory_space=pltpu.VMEM)
SMEM = pl.BlockSpec(memory_space=pltpu.SMEM)


def near(x):
    return pltpu.with_memory_space_constraint(x, pltpu.VMEM)


def to_all(x, axes, size):
    return lax.all_to_all(jnp.broadcast_to(x[None], (size, *x.shape)), axes, 0, 0, tiled=True)


def note_groups():
    groups = []
    for q in range(2):
        groups.append(
            [
                (((q ^ h) * 2 + p) * 4 + x) * 4 + h * 2 + c
                for p in range(2)
                for x in range(4)
                for h in range(2)
                for c in range(2)
            ]
        )
    return groups


SWAP = [(1, 2), (2, 1)]
ACROSS = [(0, 1), (1, 0)]


def per_device(gradients, block_layer):
    own = gradients[0, 0]
    role = lax.axis_index("c")
    keeper = role == lax.axis_index("p")
    swapped = lax.ppermute(own, CHIP_PAIR, SWAP)
    one = jnp.where(keeper, own, swapped)
    two = lax.ppermute(one, "c", ACROSS)
    packed = pl.pallas_call(
        pack_kernel,
        out_shape=pltpu.VMEM((N_PEER, 2 * BODY + DIAG, LANE), jnp.bfloat16),
        in_specs=[SMEM, VMEM, VMEM],
        out_specs=VMEM,
        name="pack",
    )(role[None], near(one), near(two))
    arrived = lax.all_to_all(packed, PEERS, 0, 0, tiled=True)
    mine = jnp.sum(arrived.astype(jnp.float32), axis=0).astype(jnp.bfloat16)
    everything = to_all(mine, PEERS, N_PEER)
    half = lax.ppermute(everything[:, BODY + DIAG :], "c", ACROSS)
    root = pl.pallas_call(
        root_kernel,
        out_shape=pltpu.VMEM((B, B), jnp.bfloat16),
        in_specs=[VMEM],
        out_specs=VMEM,
        name="root",
    )(near(everything))
    other = lax.ppermute(root, "c", ACROSS)
    place = (lax.axis_index("q") * 2 + role) * 8 + lax.axis_index("z")
    layer = jnp.where(keeper, block_layer[0], -1)
    scalars = jnp.stack([role, place, layer]).astype(jnp.int32)
    rows, note = pl.pallas_call(
        apply_kernel,
        out_shape=(
            pltpu.VMEM((ROWS, B), jnp.float32),
            pltpu.VMEM((N_NOTE, 1, LANE), jnp.float32),
        ),
        in_specs=[SMEM, VMEM, VMEM, VMEM, VMEM],
        out_specs=(VMEM, VMEM),
        scratch_shapes=[pltpu.VMEM((B, B), jnp.float32)],
        name="apply",
    )(scalars, near(everything), near(half), near(root), near(other))
    moved = lax.ppermute(rows, CHIP_PAIR, SWAP)
    notes = lax.all_to_all(note, NOTE_AXES, 0, 0, tiled=True, axis_index_groups=note_groups())
    update = pl.pallas_call(
        scale_kernel,
        out_shape=jax.ShapeDtypeStruct((ROWS, B), jnp.bfloat16),
        in_specs=[SMEM, VMEM, VMEM, VMEM],
        out_specs=VMEM,
        name="scale",
    )(jnp.stack([block_layer[0], keeper.astype(jnp.int32)]), near(notes), near(rows), near(moved))
    return update[None]


def solution(mesh):
    finer = Mesh(mesh.devices.reshape(2, 2, 8, 4, 2, 2), DP + OWNER)
    in_specs = (P(DP, OWNER, None, None), P(OWNER))
    out_specs = P(OWNER, DP, None)
    return jax.shard_map(
        per_device, mesh=finer, in_specs=in_specs, out_specs=out_specs, check_vma=False
    )
```

```python
import jax
import jax.numpy as jnp
from jax import lax
from jax.experimental import pallas as pl
from jax.experimental.pallas import tpu as pltpu
from jax.sharding import Mesh
from jax.sharding import PartitionSpec as P

DP = ("q", "p", "z")
OWNER = ("x", "h", "c")
PEERS = ("q", "z")
CHIP_PAIR = ("p", "c")
NOTE_AXES = ("q", "p", "x", "h", "c")
B = 512
H = B // 2
LANE = 128
N_DP = 32
N_PEER = 16
N_NOTE = 32
ROWS = B // N_DP
SLAB = H // N_PEER
COLS = B // LANE
BODY = SLAB * COLS
DIAG = 8


def dot(a, b, contract=((1,), (0,))):
    return lax.dot_general(a, b, (contract, ((), ())), preferred_element_type=jnp.float32)


def triangle():
    row = lax.broadcasted_iota(jnp.int32, (H, H), 0)
    col = lax.broadcasted_iota(jnp.int32, (H, H), 1)
    return row, col


def fetch_kernel(layer_ref, grad_ref, copy_ref, label_ref):
    copy_ref[...] = grad_ref[...]
    label_ref[...] = jnp.full(label_ref.shape, layer_ref[0].astype(jnp.float32), jnp.float32)


def pack_kernel(one_ref, two_ref, out_ref):
    row, col = triangle()
    own_role = lax.axis_index("c")

    def pack(role):
        upper = cross = lower = 0.0
        for ref in (one_ref, two_ref):
            if role == 0:
                first, second, contract = ref[:H], ref[H:], ((1,), (1,))
            else:
                first, second, contract = ref[:, :H], ref[:, H:], ((0,), (0,))
            upper += dot(first, first, contract)
            cross += dot(first, second, contract)
            lower += dot(second, second, contract)
        folded = jnp.where(row <= col, upper, lower).astype(jnp.bfloat16)
        cross = cross.astype(jnp.bfloat16)
        diagonal = jnp.sum(jnp.where(row == col, lower, 0.0), axis=0, keepdims=True)
        for c, part in enumerate((cross[:, :LANE], cross[:, LANE:], folded[:, :LANE], folded[:, LANE:])):
            out_ref[:, c * SLAB : (c + 1) * SLAB, :] = part.reshape(N_PEER, SLAB, LANE)
        out_ref[:, BODY : BODY + DIAG, :] = jnp.zeros((N_PEER, DIAG, LANE), jnp.bfloat16)
        extra = jnp.concatenate(
            [diagonal[:, :LANE], diagonal[:, LANE:], jnp.zeros((DIAG - 2, LANE), jnp.float32)], axis=0
        )
        out_ref[0, BODY : BODY + DIAG, :] = extra.astype(jnp.bfloat16)
        half = slice(role * H, (role + 1) * H)
        total = (one_ref[half].astype(jnp.float32) + two_ref[half].astype(jnp.float32)).astype(jnp.bfloat16)
        for c in range(COLS):
            start = BODY + DIAG + c * SLAB
            out_ref[:, start : start + SLAB, :] = total[:, c * LANE : (c + 1) * LANE].reshape(N_PEER, SLAB, LANE)

    for role in range(2):
        pl.when(own_role == role)(lambda role=role: pack(role))


def inverse_root(statistic_parts, row, col):
    upper, cross, lower = statistic_parts
    on_diagonal = row == col
    trace = jnp.sum(jnp.where(on_diagonal, upper + lower, 0.0))
    ridge = 0.01 * trace / B + 1e-06
    upper = jnp.where(on_diagonal, upper + ridge, upper)
    lower = jnp.where(on_diagonal, lower + ridge, lower)
    total = jnp.sum(upper * upper + 2.0 * (cross * cross) + lower * lower)
    total = jnp.broadcast_to(total, (1, LANE))
    inverse_scale = lax.rsqrt(total)[:, :1]
    root_scale = jnp.exp(jnp.log(total) * -0.125)[:, :1]
    current = jnp.concatenate(
        [jnp.concatenate([upper, cross], axis=1), jnp.concatenate([cross.T, lower], axis=1)], axis=0
    ) * inverse_scale

    def advance(m):
        mb = m.astype(jnp.bfloat16)
        u = dot(mb, mb) * 0.0625 - 0.625 * m
        ub = u.astype(jnp.bfloat16)
        v = dot(ub, ub) + 3.125 * u
        return mb, dot(v.astype(jnp.bfloat16), mb) + 2.44140625 * m

    mb, second = advance(current)
    sb, third = advance(second)
    y = dot(mb, sb) * 0.0625 - 0.3125 * (current + second)
    tb = third.astype(jnp.bfloat16)
    z = dot(y.astype(jnp.bfloat16), tb)
    rest = 1.25 * y - 0.390625 * third - 0.25 * z
    full_row = lax.broadcasted_iota(jnp.int32, (B, B), 0)
    full_col = lax.broadcasted_iota(jnp.int32, (B, B), 1)
    return (jnp.where(full_row == full_col, rest + 1.953125, rest) * root_scale).astype(jnp.bfloat16)


def root_kernel(stat_ref, out_ref):
    row, col = triangle()
    parts = [
        stat_ref[:, c * SLAB : (c + 1) * SLAB, :].reshape(H, LANE).astype(jnp.float32)
        for c in range(COLS)
    ]
    cross = jnp.concatenate(parts[:2], axis=1)
    folded = jnp.concatenate(parts[2:], axis=1)
    flipped = folded.T
    extra = stat_ref[0, BODY : BODY + DIAG, :].astype(jnp.float32)
    diagonal = jnp.concatenate([extra[0:1], extra[1:2]], axis=1)
    upper = jnp.where(row <= col, folded, flipped)
    lower = jnp.where(row > col, folded, flipped)
    lower = jnp.where(row == col, diagonal, lower)
    for c in range(COLS):
        start = BODY + DIAG + c * SLAB
        out_ref[B:, c * LANE : (c + 1) * LANE] = stat_ref[:, start : start + SLAB, :].reshape(H, LANE)
    out_ref[:B] = inverse_root((upper, cross, lower), row, col)


def apply_kernel(label_ref, mine_ref, other_ref, rows_ref, note_ref, whole_ref):
    role = lax.axis_index("c")
    keeper = role == lax.axis_index("p")

    def apply(left_ref, right_ref):
        middle = dot(left_ref[:B, :H], left_ref[B:]) + dot(left_ref[:B, H:], right_ref[B:])
        right = right_ref[:B]
        high = middle.astype(jnp.bfloat16)
        low = (middle - high.astype(jnp.float32)).astype(jnp.bfloat16)
        whole = (dot(high, right) + dot(low, right)) * (1.0 / N_DP)
        whole_ref[...] = whole
        energy = jnp.sum(whole * whole)
        lane = lax.broadcasted_iota(jnp.int32, note_ref.shape, 2)
        layer = jnp.where(keeper, label_ref[0:1, :], -1.0)[None]
        note_ref[...] = jnp.where(lane == 0, energy, layer)

    pl.when(role == 0)(lambda: apply(mine_ref, other_ref))
    pl.when(role == 1)(lambda: apply(other_ref, mine_ref))
    place = (lax.axis_index("q") * 2 + role) * 8 + lax.axis_index("z")
    rows_ref[...] = whole_ref[pl.ds(place * ROWS, ROWS), :]


def scale_kernel(label_ref, notes_ref, rows_ref, moved_ref, out_ref):
    keeper = lax.axis_index("c") == lax.axis_index("p")
    notes = notes_ref[...]
    mine = notes[:, 0, 1:2] == label_ref[0:1, 0:1]
    energy = jnp.sum(jnp.where(mine, notes[:, 0, 0:1], 0.0), axis=0, keepdims=True)
    count = jnp.sum(jnp.where(mine, float(B * B), 0.0), axis=0, keepdims=True)
    rows = jnp.where(keeper, rows_ref[...], moved_ref[...])
    out_ref[...] = (rows * lax.rsqrt(energy / count + 1e-06)).astype(jnp.bfloat16)


VMEM = pl.BlockSpec(memory_space=pltpu.VMEM)
SMEM = pl.BlockSpec(memory_space=pltpu.SMEM)


def near(x):
    return pltpu.with_memory_space_constraint(x, pltpu.VMEM)


def to_all(x, axes, size):
    return lax.all_to_all(jnp.broadcast_to(x[None], (size, *x.shape)), axes, 0, 0, tiled=True)


def note_groups():
    groups = []
    for q in range(2):
        groups.append(
            [
                (((q ^ h) * 2 + p) * 4 + x) * 4 + h * 2 + c
                for p in range(2)
                for x in range(4)
                for h in range(2)
                for c in range(2)
            ]
        )
    return groups


SWAP = [(1, 2), (2, 1)]
ACROSS = [(0, 1), (1, 0)]


def per_device(gradients, block_layer):
    own = gradients[0, 0]
    keeper = lax.axis_index("c") == lax.axis_index("p")
    swapped = lax.ppermute(own, CHIP_PAIR, SWAP)
    local, label = pl.pallas_call(
        fetch_kernel,
        out_shape=(pltpu.VMEM((B, B), jnp.bfloat16), pltpu.VMEM((8, LANE), jnp.float32)),
        in_specs=[SMEM, VMEM],
        out_specs=(VMEM, VMEM),
        name="fetch",
    )(block_layer, own)
    one = jnp.where(keeper, local, swapped)
    two = lax.ppermute(one, "c", ACROSS)
    packed = pl.pallas_call(
        pack_kernel,
        out_shape=pltpu.VMEM((N_PEER, 2 * BODY + DIAG, LANE), jnp.bfloat16),
        in_specs=[VMEM, VMEM],
        out_specs=VMEM,
        name="pack",
    )(near(one), near(two))
    arrived = lax.all_to_all(packed, PEERS, 0, 0, tiled=True)
    mine = jnp.sum(arrived.astype(jnp.float32), axis=0).astype(jnp.bfloat16)
    everything = to_all(mine, PEERS, N_PEER)
    solved = pl.pallas_call(
        root_kernel,
        out_shape=pltpu.VMEM((B + H, B), jnp.bfloat16),
        in_specs=[VMEM],
        out_specs=VMEM,
        name="root",
    )(near(everything))
    other = lax.ppermute(solved, "c", ACROSS)
    rows, note = pl.pallas_call(
        apply_kernel,
        out_shape=(
            pltpu.VMEM((ROWS, B), jnp.float32),
            pltpu.VMEM((N_NOTE, 1, LANE), jnp.float32),
        ),
        in_specs=[VMEM, VMEM, VMEM],
        out_specs=(VMEM, VMEM),
        scratch_shapes=[pltpu.VMEM((B, B), jnp.float32)],
        name="apply",
    )(near(label), near(solved), near(other))
    notes = lax.all_to_all(note, NOTE_AXES, 0, 0, tiled=True, axis_index_groups=note_groups())
    moved = lax.ppermute(rows, CHIP_PAIR, SWAP)
    update = pl.pallas_call(
        scale_kernel,
        out_shape=jax.ShapeDtypeStruct((ROWS, B), jnp.bfloat16),
        in_specs=[VMEM, VMEM, VMEM, VMEM],
        out_specs=VMEM,
        name="scale",
    )(near(label), near(notes), near(rows), near(moved))
    return update[None]


def solution(mesh):
    finer = Mesh(mesh.devices.reshape(2, 2, 8, 4, 2, 2), DP + OWNER)
    in_specs = (P(DP, OWNER, None, None), P(OWNER))
    out_specs = P(OWNER, DP, None)
    return jax.shard_map(
        per_device, mesh=finer, in_specs=in_specs, out_specs=out_specs, check_vma=False
    )
```

```python
import jax
import jax.numpy as jnp
from jax import lax
from jax.experimental import pallas as pl
from jax.experimental.pallas import tpu as pltpu
from jax.sharding import Mesh
from jax.sharding import PartitionSpec as P

DP = ("q", "p", "z")
OWNER = ("x", "h", "c")
PEERS = ("q", "z")
CHIP_PAIR = ("p", "c")
NOTE_AXES = ("q", "p", "x", "h")
B = 512
H = B // 2
LANE = 128
N_DP = 32
N_PEER = 16
N_NOTE = 16
ROWS = B // N_DP
SLAB = H // N_PEER
COLS = B // LANE
BODY = SLAB * COLS
DIAG = 8


def dot(a, b, contract=((1,), (0,))):
    return lax.dot_general(a, b, (contract, ((), ())), preferred_element_type=jnp.float32)


def triangle():
    row = lax.broadcasted_iota(jnp.int32, (H, H), 0)
    col = lax.broadcasted_iota(jnp.int32, (H, H), 1)
    return row, col


def fetch_kernel(layer_ref, grad_ref, copy_ref, label_ref):
    copy_ref[...] = grad_ref[...]
    label_ref[...] = jnp.full(label_ref.shape, layer_ref[0].astype(jnp.float32), jnp.float32)


def pack_kernel(one_ref, two_ref, out_ref):
    row, col = triangle()
    own_role = lax.axis_index("c")

    def pack(role):
        upper = cross = lower = 0.0
        for ref in (one_ref, two_ref):
            if role == 0:
                first, second, contract = ref[:H], ref[H:], ((1,), (1,))
            else:
                first, second, contract = ref[:, :H], ref[:, H:], ((0,), (0,))
            upper += dot(first, first, contract)
            cross += dot(first, second, contract)
            lower += dot(second, second, contract)
        folded = jnp.where(row <= col, upper, lower).astype(jnp.bfloat16)
        cross = cross.astype(jnp.bfloat16)
        diagonal = jnp.sum(jnp.where(row == col, lower, 0.0), axis=0, keepdims=True)
        for c, part in enumerate((cross[:, :LANE], cross[:, LANE:], folded[:, :LANE], folded[:, LANE:])):
            out_ref[:, c * SLAB : (c + 1) * SLAB, :] = part.reshape(N_PEER, SLAB, LANE)
        out_ref[:, BODY : BODY + DIAG, :] = jnp.zeros((N_PEER, DIAG, LANE), jnp.bfloat16)
        extra = jnp.concatenate(
            [diagonal[:, :LANE], diagonal[:, LANE:], jnp.zeros((DIAG - 2, LANE), jnp.float32)], axis=0
        )
        out_ref[0, BODY : BODY + DIAG, :] = extra.astype(jnp.bfloat16)
        half = slice(role * H, (role + 1) * H)
        total = (one_ref[half].astype(jnp.float32) + two_ref[half].astype(jnp.float32)).astype(jnp.bfloat16)
        for c in range(COLS):
            start = BODY + DIAG + c * SLAB
            out_ref[:, start : start + SLAB, :] = total[:, c * LANE : (c + 1) * LANE].reshape(N_PEER, SLAB, LANE)

    for role in range(2):
        pl.when(own_role == role)(lambda role=role: pack(role))


def inverse_root(statistic_parts, row, col):
    upper, cross, lower = statistic_parts
    on_diagonal = row == col
    trace = jnp.sum(jnp.where(on_diagonal, upper + lower, 0.0))
    ridge = 0.01 * trace / B + 1e-06
    upper = jnp.where(on_diagonal, upper + ridge, upper)
    lower = jnp.where(on_diagonal, lower + ridge, lower)
    total = jnp.sum(upper * upper + 2.0 * (cross * cross) + lower * lower)
    total = jnp.broadcast_to(total, (1, LANE))
    inverse_scale = lax.rsqrt(total)[:, :1]
    root_scale = jnp.exp(jnp.log(total) * -0.125)[:, :1]
    current = jnp.concatenate(
        [jnp.concatenate([upper, cross], axis=1), jnp.concatenate([cross.T, lower], axis=1)], axis=0
    ) * inverse_scale

    def advance(m):
        mb = m.astype(jnp.bfloat16)
        u = dot(mb, mb) * 0.0625 - 0.625 * m
        ub = u.astype(jnp.bfloat16)
        v = dot(ub, ub) + 3.125 * u
        return mb, dot(v.astype(jnp.bfloat16), mb) + 2.44140625 * m

    mb, second = advance(current)
    sb, third = advance(second)
    y = dot(mb, sb) * 0.0625 - 0.3125 * (current + second)
    tb = third.astype(jnp.bfloat16)
    z = dot(y.astype(jnp.bfloat16), tb)
    rest = 1.25 * y - 0.390625 * third - 0.25 * z
    full_row = lax.broadcasted_iota(jnp.int32, (B, B), 0)
    full_col = lax.broadcasted_iota(jnp.int32, (B, B), 1)
    return (jnp.where(full_row == full_col, rest + 1.953125, rest) * root_scale).astype(jnp.bfloat16)


def root_kernel(label_ref, stat_ref, out_ref):
    row, col = triangle()
    parts = [
        stat_ref[:, c * SLAB : (c + 1) * SLAB, :].reshape(H, LANE).astype(jnp.float32)
        for c in range(COLS)
    ]
    cross = jnp.concatenate(parts[:2], axis=1)
    folded = jnp.concatenate(parts[2:], axis=1)
    flipped = folded.T
    extra = stat_ref[0, BODY : BODY + DIAG, :].astype(jnp.float32)
    diagonal = jnp.concatenate([extra[0:1], extra[1:2]], axis=1)
    upper = jnp.where(row <= col, folded, flipped)
    lower = jnp.where(row > col, folded, flipped)
    lower = jnp.where(row == col, diagonal, lower)
    for c in range(COLS):
        start = BODY + DIAG + c * SLAB
        out_ref[B : B + H, c * LANE : (c + 1) * LANE] = stat_ref[:, start : start + SLAB, :].reshape(H, LANE)
    out_ref[B + H :, :LANE] = label_ref[...].astype(jnp.bfloat16)
    out_ref[B + H :, LANE:] = jnp.zeros((DIAG, B - LANE), jnp.bfloat16)
    out_ref[:B] = inverse_root((upper, cross, lower), row, col)


def by_role(mine_ref, other_ref, apply):
    role = lax.axis_index("c")
    pl.when(role == 0)(lambda: apply(mine_ref, other_ref))
    pl.when(role == 1)(lambda: apply(other_ref, mine_ref))


def energy_kernel(label_ref, mine_ref, other_ref, note_ref):
    keeper = lax.axis_index("c") == lax.axis_index("p")

    def apply(left_ref, right_ref):
        middle = dot(left_ref[:B, :H], left_ref[B : B + H]) + dot(left_ref[:B, H:], right_ref[B : B + H])
        whole = dot(middle.astype(jnp.bfloat16), right_ref[:B]) * (1.0 / N_DP)
        energy = jnp.sum(whole * whole)
        lane = lax.broadcasted_iota(jnp.int32, note_ref.shape, 2)
        passed = other_ref[B + H : B + H + DIAG, :LANE].astype(jnp.float32)
        layer = jnp.where(keeper, label_ref[0:1, :], passed[0:1])[None]
        note_ref[...] = jnp.where(lane == 0, energy, layer)

    by_role(mine_ref, other_ref, apply)


def rows_kernel(mine_ref, other_ref, rows_ref):
    place = (lax.axis_index("q") * 2 + lax.axis_index("c")) * 8 + lax.axis_index("z")

    def apply(left_ref, right_ref):
        left = left_ref[pl.ds(place * ROWS, ROWS), :]
        middle = dot(left[:, :H], left_ref[B : B + H]) + dot(left[:, H:], right_ref[B : B + H])
        high = middle.astype(jnp.bfloat16)
        low = (middle - high.astype(jnp.float32)).astype(jnp.bfloat16)
        both = dot(jnp.concatenate([high, low], axis=0), right_ref[:B])
        rows_ref[...] = (both[:ROWS] + both[ROWS:]) * (1.0 / N_DP)

    by_role(mine_ref, other_ref, apply)


def scale_kernel(label_ref, notes_ref, rows_ref, moved_ref, out_ref):
    keeper = lax.axis_index("c") == lax.axis_index("p")
    notes = notes_ref[...]
    mine = notes[:, 0, 1:2] == label_ref[0:1, 0:1]
    energy = jnp.sum(jnp.where(mine, notes[:, 0, 0:1], 0.0), axis=0, keepdims=True)
    count = jnp.sum(jnp.where(mine, float(B * B), 0.0), axis=0, keepdims=True)
    rows = jnp.where(keeper, rows_ref[...], moved_ref[...])
    out_ref[...] = (rows * lax.rsqrt(energy / count + 1e-06)).astype(jnp.bfloat16)


VMEM = pl.BlockSpec(memory_space=pltpu.VMEM)
SMEM = pl.BlockSpec(memory_space=pltpu.SMEM)


def near(x):
    return pltpu.with_memory_space_constraint(x, pltpu.VMEM)


def to_all(x, axes, size):
    return lax.all_to_all(jnp.broadcast_to(x[None], (size, *x.shape)), axes, 0, 0, tiled=True)


def note_groups():
    return [
        [(((q ^ h) * 2 + p) * 4 + x) * 2 + h for p in range(2) for x in range(4) for h in range(2)]
        for q in range(2)
    ]


SWAP = [(1, 2), (2, 1)]
ACROSS = [(0, 1), (1, 0)]


def per_device(gradients, block_layer):
    own = gradients[0, 0]
    keeper = lax.axis_index("c") == lax.axis_index("p")
    swapped = lax.ppermute(own, CHIP_PAIR, SWAP)
    local, label = pl.pallas_call(
        fetch_kernel,
        out_shape=(pltpu.VMEM((B, B), jnp.bfloat16), pltpu.VMEM((8, LANE), jnp.float32)),
        in_specs=[SMEM, VMEM],
        out_specs=(VMEM, VMEM),
        name="fetch",
    )(block_layer, own)
    one = jnp.where(keeper, local, swapped)
    two = lax.ppermute(one, "c", ACROSS)
    packed = pl.pallas_call(
        pack_kernel,
        out_shape=pltpu.VMEM((N_PEER, 2 * BODY + DIAG, LANE), jnp.bfloat16),
        in_specs=[VMEM, VMEM],
        out_specs=VMEM,
        name="pack",
    )(near(one), near(two))
    arrived = lax.all_to_all(packed, PEERS, 0, 0, tiled=True)
    mine = jnp.sum(arrived.astype(jnp.float32), axis=0).astype(jnp.bfloat16)
    everything = to_all(mine, PEERS, N_PEER)
    solved = pl.pallas_call(
        root_kernel,
        out_shape=pltpu.VMEM((B + H + DIAG, B), jnp.bfloat16),
        in_specs=[VMEM, VMEM],
        out_specs=VMEM,
        name="root",
    )(near(label), near(everything))
    other = lax.ppermute(solved, "c", ACROSS)
    note = pl.pallas_call(
        energy_kernel,
        out_shape=pltpu.VMEM((N_NOTE, 1, LANE), jnp.float32),
        in_specs=[VMEM, VMEM, VMEM],
        out_specs=VMEM,
        name="energy",
    )(near(label), near(solved), near(other))
    notes = lax.all_to_all(note, NOTE_AXES, 0, 0, tiled=True, axis_index_groups=note_groups())
    rows = pl.pallas_call(
        rows_kernel,
        out_shape=pltpu.VMEM((ROWS, B), jnp.float32),
        in_specs=[VMEM, VMEM],
        out_specs=VMEM,
        name="rows",
    )(near(solved), near(other))
    moved = lax.ppermute(rows, CHIP_PAIR, SWAP)
    update = pl.pallas_call(
        scale_kernel,
        out_shape=jax.ShapeDtypeStruct((ROWS, B), jnp.bfloat16),
        in_specs=[VMEM, VMEM, VMEM, VMEM],
        out_specs=VMEM,
        name="scale",
    )(near(label), near(notes), near(rows), near(moved))
    return update[None]


def solution(mesh):
    finer = Mesh(mesh.devices.reshape(2, 2, 8, 4, 2, 2), DP + OWNER)
    in_specs = (P(DP, OWNER, None, None), P(OWNER))
    out_specs = P(OWNER, DP, None)
    return jax.shard_map(
        per_device, mesh=finer, in_specs=in_specs, out_specs=out_specs, check_vma=False
    )
```
